256 devices in a mesh: cells: 128 (over y_lo, x, z, core), ens: 2 (over y_hi).
Axes of the slice: x: 4, y: 4 (y_hi: 2, y_lo: 2; y = y_hi * 2 + y_lo), z: 8, core: 2. Of those that a mesh axis runs over, the one named last changes fastest.
Arguments:
- later_adjoint: float32 [4, 4, 256, 8, 128], P('ens', None, 'cells'), may hold values from -6 to 6
- coupling: bfloat16 [4, 6, 4, 4, 256, 8, 128], P('ens', None, None, None, 'cells'), may hold values from -0.59765625 to 0.59765625
- diag_inverse: bfloat16 [4, 4, 4, 256, 8, 128], P('ens', None, None, 'cells'), may hold values from -0.7 to 1.6, as said below
- sensitivity: bfloat16 [4, 4, 256, 8, 128, 128], P('ens', None, 'cells'), may hold values from -0.0625 to 0.0625
- well_cells: int32 [256], replicated, may hold values from 0 to 262143
- well_misfit: float32 [4, 4, 256], P('ens'), may hold values from -6 to 6
- block_map: int32 [256, 8, 128], P('cells'), may hold values from 0 to 511, as said below
Outputs:
- adjoint: float32 [4, 4, 256, 8, 128], P('ens', None, 'cells')
- gradient: float32 [512, 128], P('cells')
The draws below stay inside these ranges and needn't reach their ends.
Inputs may be any that keep to these rules, and one draw needn't show every extreme that they name: `block_map`: of the cells of each slab of 2 planes along the first dimension (x from i * 2 to i * 2 + 1), exactly 16 map to blocks whose number divided by 4 (rounded down) equals any given j. `diag_inverse`: each block is the inverse of a diagonal block; its diagonal entries lie in 0.4 to 1.6. `well_cells`: wells may share a cell.
All inputs are finite; a program needn't handle non-finite values.
Results may differ from the reference program's by a relative error of at most 0.0003.
Values sent between devices are 32-bit elements; how exact they have to be, the bound alone decides.
A program may use at most 64 MiB of HBM per device.

```python
import jax
import jax.numpy as jnp
from jax import lax

UNK = 4
PBLK = 128
CX = 2
NY = 8
NZ = 128
ITERS = 4
WELLS = 256
BLK_DEV = 4
MEMBERS = 4
NX = 256
NBLK = 512
N_CELLS = 128


def draw_diag_inverse(key, part):
    shape = (MEMBERS, UNK, UNK, NX, NY, NZ)
    identity = jnp.eye(UNK, dtype=jnp.float32)[None, :, :, None, None, None]
    key_diag = jax.random.fold_in(key, 21)
    key_off = jax.random.fold_in(key, 22)
    diagonal = jax.random.uniform(key_diag, shape, jnp.float32, 0.6, 1.4)
    offdiag = jnp.clip(0.2 * jax.random.normal(key_off, shape, jnp.float32), -0.7, 0.7)
    return (identity * diagonal + (1.0 - identity) * offdiag).astype(jnp.bfloat16)


def draw_block_map(key, part):
    slab_cells = CX * NY * NZ
    per_owner = slab_cells // N_CELLS
    owners = jnp.repeat(jnp.arange(N_CELLS, dtype=jnp.int32), per_owner)
    keys = jax.random.split(jax.random.fold_in(key, 31), N_CELLS)
    shuffled = jax.vmap(lambda single: jax.random.permutation(single, owners))(keys)
    within = jax.random.randint(jax.random.fold_in(key, 32), (N_CELLS, slab_cells), 0, BLK_DEV, dtype=jnp.int32)
    return (shuffled * BLK_DEV + within).reshape(NX, NY, NZ)


def plant(entries, stream_key, low, high):
    longest = entries.shape.index(max(entries.shape))
    spots = []
    for shift in (0, 1):
        where = [jax.random.randint(jax.random.fold_in(stream_key, axis), (), 0, length) for axis, length in enumerate(entries.shape)]
        where[longest] = (where[longest] + shift) % entries.shape[longest]
        spots.append(tuple(where))
    return entries.at[spots[0]].set(low).at[spots[1]].set(high)


def level_of(rng, shape, cuts, smallest, largest):
    def one(position, blocks):
        heights = jax.random.uniform(jax.random.fold_in(jax.random.fold_in(rng, 6), position), (blocks,), jnp.float32, smallest / len(cuts), largest / len(cuts))
        return jnp.repeat(jnp.exp(heights), shape[position] // blocks).reshape((-1,) + (1,) * (len(shape) - position - 1))

    loudness = one(*cuts[0])
    for cut in cuts[1:]:
        loudness = loudness * one(*cut)
    return loudness


def scatter_about(own_key, shape, width, most, cuts=(), kind=jnp.bfloat16):
    factor_of = level_of(own_key, shape, cuts, -0.22, 0.18) if cuts else 1.0
    result = jax.random.normal(own_key, shape, jnp.float32) * width * factor_of
    return jnp.minimum(jnp.maximum(result, -most), most).astype(kind)


def setup_inputs(seed: int = 0) -> dict:
    splits = jax.random.split(jax.random.key(seed), 8)
    later_adjoint = scatter_about(splits[0], (MEMBERS, UNK, NX, NY, NZ), 1.0, 6.0, ((0, 2), (2, 128)), jnp.float32)
    coupling = scatter_about(splits[1], (MEMBERS, 6, UNK, UNK, NX, NY, NZ), 0.1, 0.59765625, ((0, 2), (4, 128)))
    diag_inverse = draw_diag_inverse(jax.random.fold_in(splits[7], 71), 0)
    sensitivity = scatter_about(splits[3], (MEMBERS, UNK, NX, NY, NZ, PBLK), (UNK * MEMBERS * CX * NY * NZ // BLK_DEV) ** -0.5, 0.0625, ((0, 2), (2, 128)))
    well_cells = plant(jax.random.randint(splits[4], (WELLS,), 0, NX * NY * NZ), jax.random.fold_in(splits[4], 1), 0, (NX * NY * NZ) - 1).astype(jnp.int32)
    well_misfit = scatter_about(splits[5], (MEMBERS, UNK, WELLS), 1.0, 6.0, ((0, 2),), jnp.float32)
    block_map = draw_block_map(jax.random.fold_in(splits[7], 71), 0)
    return {"later_adjoint": later_adjoint, "coupling": coupling, "diag_inverse": diag_inverse, "sensitivity": sensitivity, "well_cells": well_cells, "well_misfit": well_misfit, "block_map": block_map}


def move_along(field, axis, forward):
    length = field.shape[axis]
    shape = list(field.shape)
    shape[axis] = 1
    zeros = jnp.zeros(shape, jnp.float32)
    if forward:
        return jnp.concatenate([zeros, lax.slice_in_dim(field, 0, length - 1, axis=axis)], axis=axis)
    return jnp.concatenate([lax.slice_in_dim(field, 1, length, axis=axis), zeros], axis=axis)


def coupling_sum(adjoint, coupling):
    terms = jnp.sum(coupling.astype(jnp.float32) * adjoint[:, None, :, None], axis=2)
    total = jnp.zeros(adjoint.shape, jnp.float32)
    directions = [(2, True), (2, False), (3, True), (3, False), (4, True), (4, False)]
    for number, (axis, forward) in enumerate(directions):
        total = total + move_along(terms[:, number], axis, forward)
    return total


def apply_inverse(diag_inverse, source):
    return jnp.sum(diag_inverse.astype(jnp.float32) * source[:, :, None], axis=1)


def reference(later_adjoint, coupling, diag_inverse, sensitivity, well_cells, well_misfit, block_map):
    members = later_adjoint.shape[0]
    count = NX * NY * NZ
    flat = later_adjoint.reshape(members, UNK, count)
    flat = flat.at[:, :, well_cells].add(well_misfit)
    source = flat.reshape(later_adjoint.shape)
    adjoint = apply_inverse(diag_inverse, source)
    for sweep in range(ITERS):
        adjoint = apply_inverse(diag_inverse, source - coupling_sum(adjoint, coupling))
    adjoint_flat = adjoint.reshape(members, UNK, count)
    sens_flat = sensitivity.reshape(members, UNK, count, PBLK)
    cell_grad = jnp.zeros((count, PBLK), jnp.float32)
    for member in range(members):
        for unknown in range(UNK):
            cell_grad = cell_grad + adjoint_flat[member, unknown][:, None] * sens_flat[member, unknown].astype(jnp.float32)
    gradient = jax.ops.segment_sum(cell_grad, block_map.reshape(-1), num_segments=NBLK)
    return adjoint, gradient
```

```python
import jax
import jax.numpy as jnp
from jax import lax
from jax.experimental import pallas as pl
from jax.experimental.pallas import tpu as pltpu
from jax.sharding import PartitionSpec as P

ITERS = 4
MESH = pl.DeviceIdType.MESH
F32 = jnp.float32
BF16 = jnp.bfloat16


def kernel(
    later_hbm, coup_hbm, dinv_hbm, sens_hbm, well_hbm, misfit_hbm, map_hbm,
    adj_ref, grad_ref,
    later, coup, dinv, sens, well, misfit, bmap,
    onehot, rhs, total, got, mine, arrived,
    halo_out, halo_in, load_sem,
    halo_send, halo_recv, send1, recv1, send2, recv2,
):
    cell = lax.axis_index("cells")
    ens = lax.axis_index("ens")
    last = lax.axis_size("cells") - 1
    core = cell % 2
    z = (cell // 2) % 8
    x = (cell // 16) % 4
    y = cell // 64

    def first_peer(step):
        dy, dx, dc = step // 8, (step // 2) % 4, step % 2
        py, px, pc = (y + dy) % 2, (x + dx) % 4, (core + dc) % 2
        return (py * 4 + px) * 16 + z * 2 + pc, (py * 4 + px) * 2 + pc

    def second_peer(step):
        de, dz = step // 8, step % 8
        pe, pz = (ens + de) % 2, (z + dz) % 8
        return pe, cell - z * 2 + pz * 2, pz, pe * 8 + pz

    barrier = pltpu.get_barrier_semaphore()
    has_below = cell > 0
    has_above = cell < last

    @pl.when(has_below)
    def _():
        pl.semaphore_signal(barrier, inc=1, device_id={"cells": cell - 1}, device_id_type=MESH)

    @pl.when(has_above)
    def _():
        pl.semaphore_signal(barrier, inc=1, device_id={"cells": cell + 1}, device_id_type=MESH)

    for step in range(1, 16):
        pl.semaphore_signal(barrier, inc=1, device_id={"cells": first_peer(step)[0]}, device_id_type=MESH)
        pe, pc, _, _ = second_peer(step)
        pl.semaphore_signal(barrier, inc=1, device_id={"cells": pc, "ens": pe}, device_id_type=MESH)

    loads = [
        pltpu.make_async_copy(src, dst, load_sem.at[i])
        for i, (src, dst) in enumerate([
            (well_hbm, well), (misfit_hbm, misfit), (later_hbm, later), (dinv_hbm, dinv),
            (coup_hbm, coup), (map_hbm, bmap), (sens_hbm, sens),
        ])
    ]
    for load in loads:
        load.start()

    for load in loads[:4]:
        load.wait()
    slot = jnp.concatenate([well[0:1], well[1:2]], axis=1) - cell * 2048
    row = slot // 128
    inside = (slot >= 0) & (slot < 2048)
    hit_xy = (jnp.where(inside, row, -1) == lax.broadcasted_iota(jnp.int32, (16, 256), 0))
    hit_z = (slot - row * 128 == lax.broadcasted_iota(jnp.int32, (128, 256), 0))
    hit_z = jnp.where(hit_z, 1.0, 0.0).astype(BF16)
    spread = jnp.concatenate(
        [jnp.where(hit_xy, jnp.broadcast_to(misfit[m, u : u + 1], (16, 256)), 0.0) for m in range(2) for u in range(4)],
        axis=0,
    )
    injected = jnp.zeros((128, 128), F32)
    for _ in range(3):
        part = spread.astype(BF16)
        injected = injected + lax.dot_general(part, hit_z, (((1,), (1,)), ((), ())), preferred_element_type=F32)
        spread = spread - part.astype(F32)
    source = later[...] + injected.reshape(2, 4, 2, 8, 128)

    def apply_inverse(field):
        return jnp.sum(dinv[...].astype(F32) * field[:, :, None], axis=1)

    lane = lax.broadcasted_iota(jnp.int32, (16, 8, 128), 2)
    sub = lax.broadcasted_iota(jnp.int32, (16, 8, 128), 1)

    def shifted(field, axis, forward):
        flat = field.reshape(16, 8, 128)
        length = flat.shape[axis]
        index = sub if axis == 1 else lane
        moved = pltpu.roll(flat, 1 if forward else length - 1, axis)
        return jnp.where(index == (0 if forward else length - 1), 0.0, moved).reshape(field.shape)

    def products(k, adjoint):
        return jnp.sum(coup[:, k].astype(F32) * adjoint[:, :, None], axis=1)

    adjoint = apply_inverse(source)
    loads[4].wait()
    pl.semaphore_wait(barrier, 30 + has_below.astype(jnp.int32) + has_above.astype(jnp.int32))

    @pl.when(jnp.logical_not(has_below))
    def _():
        halo_in[:, 0] = jnp.zeros(halo_in[:, 0].shape, F32)

    @pl.when(jnp.logical_not(has_above))
    def _():
        halo_in[:, 1] = jnp.zeros(halo_in[:, 1].shape, F32)

    def halo_copies(sweep):
        up = pltpu.make_async_remote_copy(
            src_ref=halo_out.at[sweep, 0], dst_ref=halo_in.at[sweep, 0],
            send_sem=halo_send.at[sweep, 0], recv_sem=halo_recv.at[sweep, 0],
            device_id={"cells": jnp.minimum(cell + 1, last)}, device_id_type=MESH,
        )
        down = pltpu.make_async_remote_copy(
            src_ref=halo_out.at[sweep, 1], dst_ref=halo_in.at[sweep, 1],
            send_sem=halo_send.at[sweep, 1], recv_sem=halo_recv.at[sweep, 1],
            device_id={"cells": jnp.maximum(cell - 1, 0)}, device_id_type=MESH,
        )
        return up, down

    for sweep in range(ITERS):
        upward = products(0, adjoint)
        downward = products(1, adjoint)
        halo_out[sweep, 0] = upward[:, :, 1]
        halo_out[sweep, 1] = downward[:, :, 0]
        up, down = halo_copies(sweep)

        @pl.when(has_above)
        def _():
            up.start()

        @pl.when(has_below)
        def _():
            down.start()

        field = source
        field = field - shifted(products(2, adjoint), 1, True)
        field = field - shifted(products(3, adjoint), 1, False)
        field = field - shifted(products(4, adjoint), 2, True)
        field = field - shifted(products(5, adjoint), 2, False)
        if sweep == 0:
            loads[5].wait()
            block = bmap[...]
            place = (block // 64) * 64 + ((block // 4) % 2) * 32 + ((block // 8) % 8) * 4 + block % 4
            rows = lax.broadcasted_iota(jnp.int32, (512, 128), 0)
            for i in range(16):
                hit = jnp.broadcast_to(place[i // 8, i % 8][None, :], (512, 128)) == rows
                onehot[:, i * 128 : (i + 1) * 128] = jnp.where(hit, 1.0, 0.0).astype(BF16)

        @pl.when(has_below)
        def _():
            up.wait_recv()

        @pl.when(has_above)
        def _():
            down.wait_recv()

        low = field[:, :, 0] - downward[:, :, 1] - halo_in[sweep, 0]
        high = field[:, :, 1] - upward[:, :, 0] - halo_in[sweep, 1]
        adjoint = apply_inverse(jnp.stack([low, high], axis=2))

    adj_ref[...] = adjoint

    loads[6].wait()
    columns = [adjoint[m, u].reshape(16, 128).T for m in range(2) for u in range(4)]
    for i in range(16):
        cell_grad = jnp.zeros((128, 128), F32)
        for m in range(2):
            for u in range(4):
                cell_grad = cell_grad + columns[m * 4 + u][:, i : i + 1] * sens[m, u, i // 8, i % 8].astype(F32)
        high = cell_grad.astype(BF16)
        rhs[i * 128 : (i + 1) * 128, :128] = high
        rhs[i * 128 : (i + 1) * 128, 128:] = (cell_grad - high.astype(F32)).astype(BF16)
    both = jnp.dot(onehot[...], rhs[...], preferred_element_type=F32)
    total[...] = (both[:, :128] + both[:, 128:]).reshape(16, 32, 128)

    copies = []
    for step in range(1, 16):
        peer, piece = first_peer(step)
        copies.append(pltpu.make_async_remote_copy(
            src_ref=total.at[piece], dst_ref=got.at[step],
            send_sem=send1.at[step], recv_sem=recv1.at[step],
            device_id={"cells": peer}, device_id_type=MESH,
        ))
    for copy in copies:
        copy.start()
    partial = total[(y * 4 + x) * 2 + core]
    for step in range(1, 16):
        copies[step - 1].wait_recv()
        partial = partial + got[step]
    mine[...] = partial.reshape(8, 4, 128)

    own = ens * 8 + z
    later_copies = []
    for step in range(1, 16):
        pe, pc, pz, slot_of = second_peer(step)
        later_copies.append((pltpu.make_async_remote_copy(
            src_ref=mine.at[pz], dst_ref=arrived.at[own],
            send_sem=send2.at[step], recv_sem=recv2.at[own],
            device_id={"cells": pc, "ens": pe}, device_id_type=MESH,
        ), slot_of))
    for copy, _ in later_copies:
        copy.start()
    arrived[own] = mine[z]
    for copy, slot_of in later_copies:
        pltpu.make_async_remote_copy(
            src_ref=mine.at[0], dst_ref=arrived.at[slot_of],
            send_sem=send2.at[0], recv_sem=recv2.at[slot_of],
            device_id={"cells": cell}, device_id_type=MESH,
        ).wait_recv()
    gradient = arrived[0]
    for i in range(1, 16):
        gradient = gradient + arrived[i]
    grad_ref[...] = gradient

    for sweep in range(ITERS):
        up, down = halo_copies(sweep)

        @pl.when(has_above)
        def _():
            up.wait_send()

        @pl.when(has_below)
        def _():
            down.wait_send()

    for copy in copies:
        copy.wait_send()
    for copy, _ in later_copies:
        copy.wait_send()


def body(later_adjoint, coupling, diag_inverse, sensitivity, well_cells, well_misfit, block_map):
    any_spec = pl.BlockSpec(memory_space=pl.ANY)
    vmem = pl.BlockSpec(memory_space=pltpu.VMEM)
    args = (later_adjoint, coupling, diag_inverse, sensitivity, well_cells.reshape(2, 128), well_misfit, block_map)
    dma = pltpu.SemaphoreType.DMA
    return pl.pallas_call(
        kernel,
        out_shape=(
            jax.ShapeDtypeStruct(later_adjoint.shape, F32),
            jax.ShapeDtypeStruct((4, 128), F32),
        ),
        in_specs=[any_spec] * 7,
        out_specs=(vmem, vmem),
        scratch_shapes=[pltpu.VMEM(a.shape, a.dtype) for a in args] + [
            pltpu.VMEM((512, 2048), BF16),
            pltpu.VMEM((2048, 256), BF16),
            pltpu.VMEM((16, 32, 128), F32),
            pltpu.VMEM((16, 32, 128), F32),
            pltpu.VMEM((8, 4, 128), F32),
            pltpu.VMEM((16, 4, 128), F32),
            pltpu.VMEM((ITERS, 2, 2, 4, 8, 128), F32),
            pltpu.VMEM((ITERS, 2, 2, 4, 8, 128), F32),
            dma((7,)),
            dma((ITERS, 2)), dma((ITERS, 2)),
            dma((16,)), dma((16,)), dma((16,)), dma((16,)),
        ],
        compiler_params=pltpu.CompilerParams(collective_id=0, has_side_effects=True),
        name="adjoint_step",
    )(*args)


def solution(mesh):
    placed = (
        P("ens", None, "cells", None, None),
        P("ens", None, None, None, "cells", None, None),
        P("ens", None, None, "cells", None, None),
        P("ens", None, "cells", None, None, None),
        P(),
        P("ens", None, None),
        P("cells", None, None),
    )
    return jax.shard_map(
        body,
        mesh=mesh,
        in_specs=placed,
        out_specs=(P("ens", None, "cells", None, None), P("cells", None)),
        check_vma=False,
    )
```

```python
import jax
import jax.numpy as jnp
from jax import lax
from jax.experimental import pallas as pl
from jax.experimental.pallas import tpu as pltpu
from jax.sharding import PartitionSpec as P

MESH = pl.DeviceIdType.MESH
F32 = jnp.float32
BF16 = jnp.bfloat16
INT = jnp.int32


def kernel(
    later_hbm, coup_hbm, dinv_hbm, sens_hbm, well_hbm, misfit_hbm, map_hbm,
    adj_ref, grad_ref,
    later, coup, dinv, sens, well, misfit, bmap,
    turned, onehot, rhs, total, core_in, mixed, got, mine, arrived,
    edge_out, edge_in,
    load_sem, edge_sem, core_sem, first_sem, second_sem, token,
):
    cell = lax.axis_index("cells")
    ens = lax.axis_index("ens")
    last = lax.axis_size("cells") - 1
    core = cell % 2
    z = (cell // 2) % 8
    x = (cell // 16) % 4
    y = cell // 64

    def first_peer(step):
        return (((y + step // 4) % 2) * 4 + (x + step % 4) % 4) * 16 + z * 2 + core

    def along_z(by):
        return cell - z * 2 + ((z + by + 8) % 8) * 2

    def remote(src, dst, send, recv, **where):
        return pltpu.make_async_remote_copy(
            src_ref=src, dst_ref=dst, send_sem=send, recv_sem=recv, device_id=where, device_id_type=MESH,
        )

    def await_bytes(ref, sem):
        pltpu.make_async_copy(ref, ref, sem).wait()

    def signal(sem, **where):
        pl.semaphore_signal(sem, inc=1, device_id=where, device_id_type=MESH)

    barrier = pltpu.get_barrier_semaphore()
    has_below = cell > 0
    has_above = cell < last

    @pl.when(has_below)
    def _():
        signal(barrier, cells=cell - 1)

    @pl.when(has_above)
    def _():
        signal(barrier, cells=cell + 1)

    loads = [
        pltpu.make_async_copy(src, dst, load_sem.at[i])
        for i, (src, dst) in enumerate([
            (well_hbm, well), (misfit_hbm, misfit), (later_hbm, later), (dinv_hbm, dinv),
            (coup_hbm, coup), (map_hbm, bmap), (sens_hbm, sens),
        ])
    ]
    for load in loads:
        load.start()
    for step in range(1, 8):
        signal(barrier, cells=first_peer(step))
    signal(barrier, ens=1 - ens)
    signal(barrier, cells=along_z(1))
    signal(barrier, cells=along_z(-1))
    for load in loads[:4]:
        load.wait()
    slot = jnp.concatenate([well[0:1], well[1:2]], axis=1) - cell * 2048
    row = slot // 128
    inside = (slot >= 0) & (slot < 2048)
    hit_xy = (jnp.where(inside, row, -1) == lax.broadcasted_iota(INT, (16, 256), 0))
    hit_z = (slot - row * 128 == lax.broadcasted_iota(INT, (128, 256), 0))
    hit_z = jnp.where(hit_z, 1.0, 0.0).astype(BF16)
    spread = jnp.concatenate(
        [jnp.where(hit_xy, jnp.broadcast_to(misfit[m, u : u + 1], (16, 256)), 0.0) for m in range(2) for u in range(4)],
        axis=0,
    )
    injected = jnp.zeros((128, 128), F32)
    for _ in range(3):
        part = spread.astype(BF16)
        injected = injected + lax.dot_general(part, hit_z, (((1,), (1,)), ((), ())), preferred_element_type=F32)
        spread = spread - part.astype(F32)
    source = later[...] + injected.reshape(2, 4, 2, 8, 128)

    def apply_inverse(field):
        return jnp.sum(dinv[...].astype(F32) * field[:, :, None], axis=1)

    lane = lax.broadcasted_iota(INT, (16, 8, 128), 2)
    sub = lax.broadcasted_iota(INT, (16, 8, 128), 1)

    def shifted(field, axis, forward):
        flat = field.reshape(16, 8, 128)
        length = flat.shape[axis]
        index = sub if axis == 1 else lane
        moved = pltpu.roll(flat, 1 if forward else length - 1, axis)
        return jnp.where(index == (0 if forward else length - 1), 0.0, moved).reshape(field.shape)

    def products(k, adjoint):
        return jnp.sum(coup[:, k].astype(F32) * adjoint[:, :, None], axis=1)

    def plane_products(k, plane, values):
        return jnp.sum(coup[:, k, :, :, plane].astype(F32) * values[:, :, None], axis=1)

    def without_halo(adjoint):
        field = source
        field = field - shifted(products(2, adjoint), 1, True)
        field = field - shifted(products(3, adjoint), 1, False)
        field = field - shifted(products(4, adjoint), 2, True)
        field = field - shifted(products(5, adjoint), 2, False)
        return take_off(field, plane_products(1, 1, adjoint[:, :, 1]), plane_products(0, 0, adjoint[:, :, 0]))

    def take_off(field, low, high):
        return jnp.stack([field[:, :, 0] - low, field[:, :, 1] - high], axis=2)

    adjoint = apply_inverse(source)
    loads[4].wait()
    for side, (k, plane) in enumerate([(0, 1), (1, 0)]):
        for w in range(4):
            edge_out[side, 2 + w] = jnp.sum(
                dinv[:, w, :, plane].astype(F32)[:, :, None] * coup[:, k, :, :, plane].astype(F32), axis=1
            )
    pl.semaphore_wait(barrier, 10 + has_below.astype(INT) + has_above.astype(INT))
    signal(token.at[0], cells=along_z(1))
    signal(token.at[0], cells=along_z(-1))

    @pl.when(jnp.logical_not(has_below))
    def _():
        edge_in[0] = jnp.zeros(edge_in[0].shape, F32)

    @pl.when(jnp.logical_not(has_above))
    def _():
        edge_in[1] = jnp.zeros(edge_in[1].shape, F32)

    def send_edges(slots, sem):
        @pl.when(has_above)
        def _():
            remote(edge_out.at[0, slots], edge_in.at[0, slots], load_sem.at[0], edge_sem.at[0, sem], cells=jnp.minimum(cell + 1, last)).start()

        @pl.when(has_below)
        def _():
            remote(edge_out.at[1, slots], edge_in.at[1, slots], load_sem.at[1], edge_sem.at[1, sem], cells=jnp.maximum(cell - 1, 0)).start()

    def await_edges(slots, sem):
        @pl.when(has_below)
        def _():
            await_bytes(edge_in.at[0, slots], edge_sem.at[0, sem])

        @pl.when(has_above)
        def _():
            await_bytes(edge_in.at[1, slots], edge_sem.at[1, sem])

    for turn in range(2):
        at = turn * 6
        upward = plane_products(0, 1, adjoint[:, :, 1])
        downward = plane_products(1, 0, adjoint[:, :, 0])
        edge_out[0, at] = upward
        edge_out[1, at] = downward
        send_edges(pl.ds(at, 1), turn * 2)
        if turn == 0:
            send_edges(pl.ds(2, 4), 1)
        field = without_halo(adjoint)
        alone = apply_inverse(field)
        edge_out[0, at + 1] = plane_products(0, 1, alone[:, :, 1])
        edge_out[1, at + 1] = plane_products(1, 0, alone[:, :, 0])
        send_edges(pl.ds(at + 1, 1), turn * 2 + 1)
        if turn == 0:
            loads[5].wait()
            block = bmap[...]
            place = (
                (((block // 4) % 2 + core) % 2) * 256
                + ((block // 256 + y) % 2) * 128
                + (((block // 64) % 4 - x + 4) % 4) * 32
                + (((block // 8) % 8 - z + 14) % 8) * 4
                + block % 4
            )
            rows = lax.broadcasted_iota(INT, (512, 128), 0)
            for i in range(16):
                hit = jnp.broadcast_to(place[i // 8, i % 8][None, :], (512, 128)) == rows
                onehot[:, i * 128 : (i + 1) * 128] = jnp.where(hit, 1.0, 0.0).astype(BF16)
            loads[6].wait()

            def turn_over(i, carry):
                for mu in range(8):
                    turned[mu, i] = sens[mu, i].T
                return carry

            lax.fori_loop(0, 16, turn_over, 0, unroll=4)
        await_edges(pl.ds(at, 1), turn * 2)
        adjoint = apply_inverse(take_off(field, edge_in[0, at], edge_in[1, at]))
        field = without_halo(adjoint)
        pl.semaphore_wait(token.at[turn], 2)
        if turn == 0:
            signal(token.at[1], cells=along_z(2))
            signal(token.at[1], cells=along_z(-2))
        else:
            signal(token.at[2], ens=1 - ens)
        await_edges(pl.ds(1, 5) if turn == 0 else pl.ds(7, 1), turn * 2 + 1)
        low = edge_in[0, at + 1]
        high = edge_in[1, at + 1]
        for w in range(4):
            low = low - edge_in[0, 2 + w] * downward[:, w][:, None]
            high = high - edge_in[1, 2 + w] * upward[:, w][:, None]
        adjoint = apply_inverse(take_off(field, low, high))

    adj_ref[...] = adjoint
    for i in range(16):
        cell_grad = jnp.zeros((128, 128), F32)
        for m in range(2):
            for u in range(4):
                weight = jnp.broadcast_to(adj_ref[m, u, i // 8, i % 8 : i % 8 + 1], (128, 128))
                cell_grad = cell_grad + weight * turned[m * 4 + u, i].astype(F32)
        top = cell_grad.astype(BF16)
        rhs[:128, i * 128 : (i + 1) * 128] = top
        rhs[128:, i * 128 : (i + 1) * 128] = (cell_grad - top.astype(F32)).astype(BF16)
    def gather(rows):
        both = lax.dot_general(onehot[rows], rhs[...], (((1,), (1,)), ((), ())), preferred_element_type=F32)
        return (both[:, :128] + both[:, 128:]).reshape(8, 2, 16, 128)

    total[1] = gather(slice(256, 512))
    swap = remote(
        total.at[1], core_in, load_sem.at[2], core_sem,
        cells=cell + 1 - 2 * core,
    )
    swap.start()
    total[0] = gather(slice(0, 256))
    swap.wait_recv()
    for half in range(2):
        for step in range(8):
            mixed[half, step] = total[0, step, half] + core_in[step, half]
        for step in (6, 2, 5, 7, 1, 3, 4):
            remote(
                mixed.at[half, step], got.at[half, step - 1], load_sem.at[3], first_sem.at[half],
                cells=first_peer(step),
            ).start()
    pl.semaphore_wait(token.at[2], 1)
    own = ens * 8 + z
    for half in range(2):
        await_bytes(got.at[half], first_sem.at[half])
        partial = mixed[half, 0]
        for step in range(7):
            partial = partial + got[half, step]
        mine[half] = partial.reshape(4, 4, 128)
        for piece in ((2, 1, 3, 0), (0, 3, 1, 2))[half]:
            by = half * 4 + piece + 2
            for de in (1, 0):
                if by == 8 and de == 0:
                    arrived[own] = mine[half, piece]
                else:
                    remote(
                        mine.at[half, piece], arrived.at[own], load_sem.at[4], second_sem,
                        cells=along_z(by - 8), ens=(ens + de) % 2,
                    ).start()
    await_bytes(arrived.at[pl.ds(0, 15)], second_sem)
    gradient = arrived[0]
    for i in range(1, 16):
        gradient = gradient + arrived[i]
    grad_ref[...] = gradient

    @pl.when(has_above)
    def _():
        await_bytes(edge_out.at[0], load_sem.at[0])

    @pl.when(has_below)
    def _():
        await_bytes(edge_out.at[1], load_sem.at[1])

    swap.wait_send()
    await_bytes(got, load_sem.at[3])
    await_bytes(arrived.at[pl.ds(0, 15)], load_sem.at[4])


def writer(adj_ref, grad_ref, adj_out, grad_out, sem):
    copies = [
        pltpu.make_async_copy(src, dst, sem.at[i])
        for i, (src, dst) in enumerate([(adj_ref, adj_out), (grad_ref, grad_out)])
    ]
    for copy in copies:
        copy.start()
    for copy in copies:
        copy.wait()


def body(later_adjoint, coupling, diag_inverse, sensitivity, well_cells, well_misfit, block_map):
    any_spec = pl.BlockSpec(memory_space=pl.ANY)
    vmem = pl.BlockSpec(memory_space=pltpu.VMEM)
    args = (
        later_adjoint, coupling, diag_inverse, sensitivity.reshape(8, 16, 128, 128),
        well_cells.reshape(2, 128), well_misfit, block_map,
    )
    dma = pltpu.SemaphoreType.DMA
    adjoint, gradient = pl.pallas_call(
        kernel,
        out_shape=(pltpu.VMEM(later_adjoint.shape, F32), pltpu.VMEM((4, 128), F32)),
        in_specs=[any_spec] * 7,
        out_specs=(vmem, vmem),
        scratch_shapes=[pltpu.VMEM(a.shape, a.dtype) for a in args] + [
            pltpu.VMEM((8, 16, 128, 128), BF16),
            pltpu.VMEM((512, 2048), BF16),
            pltpu.VMEM((256, 2048), BF16),
            pltpu.VMEM((2, 8, 2, 16, 128), F32),
            pltpu.VMEM((8, 2, 16, 128), F32),
            pltpu.VMEM((2, 8, 16, 128), F32),
            pltpu.VMEM((2, 7, 16, 128), F32),
            pltpu.VMEM((2, 4, 4, 128), F32),
            pltpu.VMEM((16, 4, 128), F32),
            pltpu.VMEM((2, 8, 2, 4, 8, 128), F32),
            pltpu.VMEM((2, 8, 2, 4, 8, 128), F32),
            dma((7,)), dma((2, 4)), dma(()), dma((2,)), dma(()),
            pltpu.SemaphoreType.REGULAR((3,)),
        ],
        compiler_params=pltpu.CompilerParams(collective_id=0, has_side_effects=True),
        name="adjoint_step",
    )(*args)
    return pl.pallas_call(
        writer,
        out_shape=(
            jax.ShapeDtypeStruct(adjoint.shape, F32),
            jax.ShapeDtypeStruct(gradient.shape, F32),
        ),
        in_specs=[any_spec, any_spec],
        out_specs=(any_spec, any_spec),
        scratch_shapes=[dma((2,))],
        name="write_out",
    )(*(pltpu.with_memory_space_constraint(a, pltpu.VMEM) for a in (adjoint, gradient)))


def solution(mesh):
    placed = (
        P("ens", None, "cells", None, None),
        P("ens", None, None, None, "cells", None, None),
        P("ens", None, None, "cells", None, None),
        P("ens", None, "cells", None, None, None),
        P(),
        P("ens", None, None),
        P("cells", None, None),
    )
    return jax.shard_map(
        body,
        mesh=mesh,
        in_specs=placed,
        out_specs=(P("ens", None, "cells", None, None), P("cells", None)),
        check_vma=False,
    )
```
